32 devices in a mesh: row: 2 (over x), col: 16 (over z, y, core).
Axes of the slice: x: 2, y: 2, z: 4, core: 2. Of those that a mesh axis runs over, the one named last changes fastest.
Arguments:
- adjacency: int32 [2048, 64], P('row', 'col'), may hold values from -2147483648 to 2147483647, as said below
- tile_mask: int32 [16, 16], P('row', 'col'), may hold values from 0 to 1, as said below
- thresholds: int32 [3], replicated, may hold values from 30 to 61
Outputs:
- truss_support: float32 [2048, 2048], P('row', 'col')
- edge_counts: int32 [3], replicated
The draws below stay inside these ranges and needn't reach their ends.
Inputs may be any that keep to these rules, and one draw needn't show every extreme that they name: The graph of adjacency is symmetric with an empty diagonal: bit b of word w of row i equals the bit for row 32 w + b and column i. `tile_mask`: Symmetric.
All inputs are finite; a program needn't handle non-finite values.
Results may differ from the reference program's by a relative error of at most 0.0003.
Values may be sent and summed in bfloat16 or wider, within the bound.
A program may use at most 64 MiB of HBM per device.

```python
import jax
import jax.numpy as jnp

TILE = 128
ITERS = 3
VERT = 2048


def draw_tile_mask(key, part):
    tiles = VERT // TILE
    base_group = jax.random.randint(jax.random.fold_in(key, 11), (tiles,), 0, 4)
    chooser = jax.random.randint(jax.random.fold_in(key, 12), (tiles,), 0, 3)
    community = jnp.where(chooser == 0, base_group, 0)
    extra_links = jax.random.randint(jax.random.fold_in(key, 13), (tiles, tiles), 0, 10)
    extra_links = jnp.minimum(extra_links, extra_links.T)
    same_group = community[:, None] == community[None, :]
    return jnp.where(same_group | (extra_links < 2), 1, 0).astype(jnp.int32)


def draw_adjacency(key, part):
    tiles = VERT // TILE
    density = jax.random.randint(jax.random.fold_in(key, 21), (tiles, tiles), 30, 400)
    density = (density + density.T) // 2
    level = jnp.repeat(jnp.repeat(density, TILE, axis=0), TILE, axis=1)
    roll = jax.random.randint(jax.random.fold_in(key, 22), (VERT, VERT), 0, 1000)
    vertex = jnp.arange(VERT, dtype=jnp.int32)
    upper = (roll < level) & (vertex[:, None] < vertex[None, :])
    full_graph = (upper | upper.T).astype(jnp.int32)
    shifts = jnp.arange(32, dtype=jnp.int32)
    shifted = jnp.left_shift(full_graph.reshape(VERT, VERT // 32, 32), shifts)
    return jnp.sum(shifted, axis=-1, dtype=jnp.int32).astype(jnp.int32)


def setup_inputs(seed: int = 0) -> dict:
    key_of = jax.random.split(jax.random.key(seed), 4)
    adjacency = draw_adjacency(jax.random.fold_in(key_of[3], 71), 0)
    tile_mask = draw_tile_mask(jax.random.fold_in(key_of[3], 71), 0)
    thresholds = jax.random.randint(key_of[2], (ITERS,), VERT * 15 // 1000, VERT * 30 // 1000 + 1).astype(jnp.int32)
    return dict(adjacency=adjacency, tile_mask=tile_mask, thresholds=thresholds)


def unpack_bits(packed_rows):
    shifts = jnp.arange(32, dtype=jnp.int32)
    flat_bits = jnp.bitwise_and(jnp.right_shift(packed_rows[:, :, None], shifts), 1)
    return flat_bits.reshape(packed_rows.shape[0], packed_rows.shape[1] * 32).astype(jnp.int32)


def reference(adjacency, tile_mask, thresholds):
    flat_bits = unpack_bits(adjacency)
    tile_cover = jnp.repeat(jnp.repeat(tile_mask, TILE, axis=0), TILE, axis=1).astype(jnp.int32)
    surviving = flat_bits * tile_cover
    survived_list = []
    support = jnp.zeros(surviving.shape, jnp.float32)
    for iteration in range(ITERS):
        operand = surviving.astype(jnp.bfloat16)
        wedge_counts = jnp.dot(operand, operand, preferred_element_type=jnp.float32)
        support = wedge_counts * surviving.astype(jnp.float32)
        retained = (support >= thresholds[iteration].astype(jnp.float32)).astype(jnp.int32)
        surviving = surviving * retained
        survived_list.append(jnp.sum(surviving).astype(jnp.int32))
    truss_support = support * surviving.astype(jnp.float32) / thresholds[ITERS - 1].astype(jnp.float32)
    return truss_support, jnp.stack(survived_list).astype(jnp.int32)
```

```python
import functools

import jax
import jax.numpy as jnp
from jax import lax
from jax.experimental import pallas as pl
from jax.experimental.pallas import tpu as pltpu
from jax.sharding import PartitionSpec as P

TILE = 128
ITERS = 3
BITS = 32
MESH = pl.DeviceIdType.MESH


def unpack_words(load_row, words, width, dtype):
    bit = lax.broadcasted_iota(jnp.int32, (BITS, width), 0)
    parts = []
    for w in range(words):
        row = jnp.broadcast_to(load_row(w), (BITS, width))
        parts.append(jnp.bitwise_and(jnp.right_shift(row, bit), 1).astype(jnp.float32).astype(dtype))
    return parts


def kernel(
    n_row, n_col, adj_ref, mask_ref, thr_ref, out_ref, count_ref,
    gath, cross, lhs, rhs, acc, live, tally, tallies,
    send_a, recv_a, send_f, recv_f, send_x, recv_x, send_c, recv_c,
):
    words, rows = adj_ref.shape
    cols = words * BITS
    pairs = n_col // 2
    n_dev = n_row * n_col
    my_row, my_col = lax.axis_index("row"), lax.axis_index("col")
    my_pair, my_core = my_col // 2, lax.rem(my_col, 2)
    me = my_row * n_col + my_col
    tiles_here = rows // TILE

    def device(flat):
        return (flat // n_col, lax.rem(flat, n_col))

    barrier = pltpu.get_barrier_semaphore()

    def greet(d, c):
        pl.semaphore_signal(
            barrier, inc=1, device_id=device(lax.rem(me + d, n_dev)), device_id_type=MESH
        )
        return c

    lax.fori_loop(1, n_dev, greet, 0)

    def keep_own(t, w, value):
        gath[t, my_col, w : w + 1, :] = value
        cross[t, my_row, w : w + 1, :] = value

    for w in range(words):
        keep_own(
            0, w,
            jnp.concatenate(
                [adj_ref[w : w + 1, i * TILE : (i + 1) * TILE] * mask_ref[i, 0] for i in range(tiles_here)],
                axis=1,
            ),
        )
    tally[...] = jnp.zeros_like(tally)
    pl.semaphore_wait(barrier, n_dev - 1)

    def direct(t, d):
        return pltpu.make_async_remote_copy(
            src_ref=gath.at[t, my_col], dst_ref=gath.at[t, my_col],
            send_sem=send_a.at[t, d], recv_sem=recv_a.at[t, d],
            device_id=(my_row, lax.rem(my_pair + d, pairs) * 2 + my_core), device_id_type=MESH,
        )

    def forward(t, d):
        slot = lax.rem(my_pair - d + pairs, pairs) * 2 + my_core
        return pltpu.make_async_remote_copy(
            src_ref=gath.at[t, slot], dst_ref=gath.at[t, slot],
            send_sem=send_f.at[t, d], recv_sem=recv_f.at[t, d],
            device_id=(my_row, my_pair * 2 + 1 - my_core), device_id_type=MESH,
        )

    def across(t, d):
        return pltpu.make_async_remote_copy(
            src_ref=gath.at[t, my_col], dst_ref=cross.at[t, my_row],
            send_sem=send_x.at[t, d], recv_sem=recv_x.at[t, d],
            device_id=(lax.rem(my_row + d, n_row), my_col), device_id_type=MESH,
        )

    def distance(k):
        odd = lax.rem(k, 2)
        return odd * ((k + 1) // 2) + (1 - odd) * (pairs - k // 2)

    def multiply(t, d):
        pair = lax.rem(my_pair - d + pairs, pairs)
        for core in range(2):
            slot = pair * 2 + core
            parts = unpack_words(lambda w: gath[t, slot, w : w + 1, :], words, rows, jnp.bfloat16)
            for w in range(words):
                rhs[core * cols + w * BITS : core * cols + (w + 1) * BITS, :] = parts[w]
        return jnp.dot(lhs[pair], rhs[...], preferred_element_type=jnp.float32)

    for t in range(ITERS):
        threshold = thr_ref[t].astype(jnp.float32)
        for d in range(1, n_row):
            across(t, d).start()
        forward(t, 0).start()

        def send(k, c):
            direct(t, distance(pairs - k)).start()
            return c

        lax.fori_loop(1, pairs, send, 0)

        parts = unpack_words(lambda w: gath[t, my_col, w : w + 1, :], words, rows, jnp.float32)
        for w in range(words):
            live[w * BITS : (w + 1) * BITS, :] = parts[w]
        for d in range(1, n_row):
            across(t, d).wait_recv()
        wide = 2 * cols
        for r in range(n_row):
            parts = unpack_words(lambda w: cross[t, r, w : w + 1, :], words, rows, jnp.bfloat16)
            for w in range(words):
                for q in range(rows // wide):
                    lhs[r * (rows // wide) + q, w * BITS : (w + 1) * BITS, :] = parts[w][:, q * wide : (q + 1) * wide]

        def arrive(k):
            d = distance(k)
            direct(t, d).wait_recv()
            forward(t, d).start()

        arrive(1)
        forward(t, 0).wait_recv()
        acc[...] = multiply(t, 0)

        def step(k, c):
            arrive(k + 1)
            forward(t, distance(k)).wait_recv()
            acc[...] += multiply(t, distance(k))
            return c

        lax.fori_loop(1, pairs - 1, step, 0)
        forward(t, distance(pairs - 1)).wait_recv()
        acc[...] += multiply(t, distance(pairs - 1))

        support = acc[...] * live[...]
        kept = jnp.where(support >= threshold, live[...], 0.0)
        if t < ITERS - 1:
            bit = jnp.left_shift(1, lax.broadcasted_iota(jnp.int32, (BITS, rows), 0))
            for w in range(words):
                own = kept[w * BITS : (w + 1) * BITS, :].astype(jnp.int32) * bit
                keep_own(t + 1, w, jnp.sum(own, axis=0, keepdims=True))
        per_row = jnp.sum(kept, axis=0, keepdims=True)
        lanes = per_row[:, :TILE]
        for i in range(1, tiles_here):
            lanes = lanes + per_row[:, i * TILE : (i + 1) * TILE]
        tally[t : t + 1, :] = lanes.astype(jnp.int32)

    def count(d):
        return pltpu.make_async_remote_copy(
            src_ref=tally, dst_ref=tallies.at[me],
            send_sem=send_c.at[d], recv_sem=recv_c.at[d],
            device_id=device(lax.rem(me + d, n_dev)), device_id_type=MESH,
        )

    def send_count(d, c):
        count(n_dev - d).start()
        return c

    lax.fori_loop(1, n_dev, send_count, 0)
    tallies[me] = tally[...]
    ratio = support * kept / threshold
    for i in range(tiles_here):
        out_ref[i * TILE : (i + 1) * TILE, :] = ratio[:, i * TILE : (i + 1) * TILE].T

    def finish_count(d, c):
        count(d).wait()
        return c

    for t in range(ITERS):
        for d in range(1, n_row):
            across(t, d).wait_send()
        forward(t, 0).wait_send()

        def finish(d, c):
            direct(t, d).wait_send()
            forward(t, d).wait_send()
            return c

        lax.fori_loop(1, pairs, finish, 0)
    lax.fori_loop(1, n_dev, finish_count, 0)
    total = jnp.sum(tallies[...], axis=0)
    for t in range(ITERS):
        count_ref[t] = jnp.sum(total[t : t + 1, :])


def local(n_row, n_col, adjacency, tile_mask, thresholds):
    packed = adjacency.T
    words, rows = packed.shape
    cols = words * BITS
    n_dev = n_row * n_col
    pairs = n_col // 2
    dma = pltpu.SemaphoreType.DMA
    return pl.pallas_call(
        functools.partial(kernel, n_row, n_col),
        out_shape=(
            jax.ShapeDtypeStruct((rows, cols), jnp.float32),
            jax.ShapeDtypeStruct((ITERS,), jnp.int32),
        ),
        in_specs=[
            pl.BlockSpec(memory_space=pltpu.VMEM),
            pl.BlockSpec(memory_space=pltpu.SMEM),
            pl.BlockSpec(memory_space=pltpu.SMEM),
        ],
        out_specs=(
            pl.BlockSpec(memory_space=pltpu.VMEM),
            pl.BlockSpec(memory_space=pltpu.SMEM),
        ),
        scratch_shapes=[
            pltpu.VMEM((ITERS, n_col, words, rows), jnp.int32),
            pltpu.VMEM((ITERS, n_row, words, rows), jnp.int32),
            pltpu.VMEM((pairs, cols, 2 * cols), jnp.bfloat16),
            pltpu.VMEM((2 * cols, rows), jnp.bfloat16),
            pltpu.VMEM((cols, rows), jnp.float32),
            pltpu.VMEM((cols, rows), jnp.float32),
            pltpu.VMEM((8, TILE), jnp.int32),
            pltpu.VMEM((n_dev, 8, TILE), jnp.int32),
            dma((ITERS, pairs)), dma((ITERS, pairs)),
            dma((ITERS, pairs)), dma((ITERS, pairs)),
            dma((ITERS, n_row)), dma((ITERS, n_row)),
            dma((n_dev,)), dma((n_dev,)),
        ],
        compiler_params=pltpu.CompilerParams(collective_id=0, has_side_effects=True),
    )(packed, tile_mask, thresholds)


def solution(mesh):
    in_specs = (P("row", "col"), P("row", "col"), P())
    out_specs = (P("row", "col"), P())
    body = functools.partial(local, mesh.shape["row"], mesh.shape["col"])
    return jax.shard_map(body, mesh=mesh, in_specs=in_specs, out_specs=out_specs, check_vma=False)
```
